32 devices in a mesh: plant: 2 (over x), section: 16 (over z, y, core).
Axes of the slice: x: 2, y: 2, z: 4, core: 2. Of those that a mesh axis runs over, the one named last changes fastest.
Arguments:
- dynamics_operator: bfloat16 [1024, 512], P('plant'), parts along dimension 0
- control_gain_array: bfloat16 [1024, 256], P('plant'), parts along dimension 0
- kkt_inverse: bfloat16 [1536, 768], P('plant'), parts along dimension 0
- lin_state: float32 [1024, 4096], P(('plant', 'section')), parts along dimension 0, may hold values from -6 to 6
- lin_input: float32 [512, 4096], P(('plant', 'section')), parts along dimension 0, may hold values from -6 to 6
- block_start: int32 [2], P('plant'), parts along dimension 0, may hold values from 0 to 15
- period: int32 [2], P('plant'), parts along dimension 0, may hold values from 2048 to 4096
Outputs:
- state_traj: float32 [1024, 4096], P('plant', 'section'), parts along dimension 0
- input_traj: float32 [512, 4096], P('plant', 'section'), parts along dimension 0
- consensus: float32 [1024, 4096], P('plant', 'section'), parts along dimension 0
- residual_norms: float32 [4], P('plant'), parts along dimension 0
The draws below stay inside these ranges and needn't reach their ends.
There are 2 independent parts, one for each index of `plant`. The reference program is written for one: setup_inputs(seed, part) draws one part's arguments, and reference() takes and returns one part's arrays. A program takes and returns all parts, laid end to end along the dimension named above; each array names one. Nothing has to cross between parts.
Inputs may be any that keep to these rules, and one draw needn't show every extreme that they name: Device d of the section axis holds the block of logical sections starting at 256 * ((d - block_start) mod the axis's size).
All inputs are finite; a program needn't handle non-finite values.
Results may differ from the reference program's by a relative error of at most 0.0045.
Values sent between devices are 32-bit elements; how exact they have to be, the bound alone decides.
A program may use at most 64 MiB of HBM per device.

```python
import jax
import jax.numpy as jnp
from jax import lax

STATE = 512
INPUT = 256
ITERS = 4
SECTIONS = 4096
N_SECTION = 16


RHO = 1.0


def plant_system(key):
    key_a = jax.random.fold_in(key, 11)
    key_b = jax.random.fold_in(key, 23)
    key_state = jax.random.fold_in(key, 37)
    key_input = jax.random.fold_in(key, 41)
    dynamics_operator = (jax.random.normal(key_a, (STATE, STATE), jnp.float32) / jnp.sqrt(jnp.float32(STATE))).astype(jnp.bfloat16)
    control_gain_array = (jax.random.normal(key_b, (STATE, INPUT), jnp.float32) / jnp.sqrt(jnp.float32(INPUT))).astype(jnp.bfloat16)
    low_end, high_end = (0.5, 5.0)
    state_weight = jnp.exp(jax.random.uniform(key_state, (STATE,), jnp.float32, jnp.log(low_end), jnp.log(high_end)))
    input_weight = jnp.exp(jax.random.uniform(key_input, (INPUT,), jnp.float32, jnp.log(0.1), jnp.log(1.0)))
    merged_pieces = jnp.concatenate([dynamics_operator, control_gain_array], axis=1).astype(jnp.float32)
    hessian = RHO * jnp.dot(merged_pieces.T, merged_pieces, precision=lax.Precision.HIGHEST)
    hessian = hessian + jnp.diag(jnp.concatenate([state_weight + RHO, input_weight]))
    inverse = jnp.linalg.inv(hessian)
    return (dynamics_operator, control_gain_array, inverse.astype(jnp.bfloat16))


def draw_dynamics_operator(key, part):
    return plant_system(key)[0]


def draw_control_gain_array(key, part):
    return plant_system(key)[1]


def draw_kkt_inverse(key, part):
    return plant_system(key)[2]


def levels(stream_key, shape, cuts, smallest, largest):
    def one(position, shards_of):
        steps = jax.random.uniform(jax.random.fold_in(jax.random.fold_in(stream_key, 6), position), (shards_of,), jnp.float32, smallest / len(cuts), largest / len(cuts))
        return jnp.repeat(jnp.exp(steps), shape[position] // shards_of).reshape((-1,) + (1,) * (len(shape) - position - 1))

    loudness = one(*cuts[0])
    for cut in cuts[1:]:
        loudness = loudness * one(*cut)
    return loudness


def noise(rng, shape, scale, most, split=(), kind=jnp.bfloat16):
    factor_of = levels(rng, shape, split, -0.22, 0.18) if split else 1.0
    entries = jax.random.normal(rng, shape, jnp.float32) * scale * factor_of
    return jnp.minimum(jnp.maximum(entries, -most), most).astype(kind)


def setup_inputs(seed: int = 0, part: int = 0) -> dict:
    key_of = jax.random.split(jax.random.key(seed), 8)
    own_keys = jax.random.split(jax.random.fold_in(key_of[7], part), 8)
    return {
        "dynamics_operator": draw_dynamics_operator(jax.random.fold_in(jax.random.fold_in(key_of[7], part), 71), part),
        "control_gain_array": draw_control_gain_array(jax.random.fold_in(jax.random.fold_in(key_of[7], part), 71), part),
        "kkt_inverse": draw_kkt_inverse(jax.random.fold_in(jax.random.fold_in(key_of[7], part), 71), part),
        "lin_state": noise(own_keys[3], (STATE, SECTIONS), 1.0, 6.0, ((0, 16),), jnp.float32),
        "lin_input": noise(own_keys[4], (INPUT, SECTIONS), 1.0, 6.0, ((0, 16),), jnp.float32),
        "block_start": jax.random.randint(own_keys[5], (1,), 0, N_SECTION).astype(jnp.int32),
        "period": jax.random.randint(own_keys[6], (1,), SECTIONS // 2, SECTIONS + 1).astype(jnp.int32),
    }


RHO = 1.0

def adjoint(dynamics_operator, control_gain_array, target):
    rounded = target.astype(jnp.bfloat16)
    contract = (((0,), (0,)), ((), ()))
    upper_part = lax.dot_general(dynamics_operator.astype(jnp.float32), rounded.astype(jnp.float32), contract, preferred_element_type=jnp.float32)
    lower_part = lax.dot_general(control_gain_array.astype(jnp.float32), rounded.astype(jnp.float32), contract, preferred_element_type=jnp.float32)
    return jnp.concatenate([upper_part, lower_part], axis=0)

def estimate_condition(dynamics_operator, control_gain_array, merged_pieces, condition_lines):
    rounded = merged_pieces.astype(jnp.bfloat16)
    return jnp.dot(dynamics_operator.astype(jnp.float32), rounded[:condition_lines].astype(jnp.float32), preferred_element_type=jnp.float32) + jnp.dot(control_gain_array.astype(jnp.float32), rounded[condition_lines:].astype(jnp.float32), preferred_element_type=jnp.float32)

def reference(dynamics_operator, control_gain_array, kkt_inverse, lin_state, lin_input, block_start, period):
    condition_lines = dynamics_operator.shape[0]
    block_width = lin_state.shape[1] // N_SECTION
    offset = (block_start[0] * block_width).astype(jnp.int32)
    neg_cost = -jnp.concatenate([jnp.roll(lin_state, -offset, 1), jnp.roll(lin_input, -offset, 1)], axis=0)
    section_total = neg_cost.shape[1]
    section_ids = jnp.arange(section_total, dtype=jnp.int32)
    working_segment = (section_ids < period[0])[None, :]
    is_first = (section_ids == 0)[None, :]
    stop_index = (period[0] - 1).astype(jnp.int32)
    is_last = (section_ids == stop_index)[None, :]
    zero_block = jnp.zeros((condition_lines, section_total), jnp.float32)
    input_zero = jnp.zeros((neg_cost.shape[0] - condition_lines, section_total), jnp.float32)
    consensus = zero_block
    dual_state = zero_block
    multiplier_link = zero_block
    ahead_z = zero_block
    feasibility_gap_total = jnp.float32(0.0)
    dual_sum = jnp.float32(0.0)
    merged_pieces = jnp.zeros_like(neg_cost)
    for iteration in range(ITERS):
        right_side = neg_cost + RHO * jnp.concatenate([consensus - dual_state, input_zero], axis=0) + RHO * adjoint(dynamics_operator, control_gain_array, ahead_z - multiplier_link)
        product = jnp.dot(kkt_inverse.astype(jnp.float32), right_side.astype(jnp.bfloat16).astype(jnp.float32), preferred_element_type=jnp.float32)
        merged_pieces = jnp.where(working_segment, product, 0.0)
        expected_condition = estimate_condition(dynamics_operator, control_gain_array, merged_pieces, condition_lines)
        own_sum = merged_pieces[:condition_lines] + dual_state
        passed_quantity = expected_condition + multiplier_link
        previous = jnp.roll(passed_quantity, 1, axis=1)
        closing_carried = lax.dynamic_slice_in_dim(passed_quantity, stop_index, 1, 1)
        previous = jnp.where(is_first, closing_carried, previous)
        newest_agreement = jnp.where(working_segment, 0.5 * (own_sum + previous), 0.0)
        onward_refreshed = jnp.where(is_last, newest_agreement[:, 0:1], jnp.roll(newest_agreement, -1, axis=1))
        change_z = newest_agreement - consensus
        dual_state = jnp.where(working_segment, dual_state + merged_pieces[:condition_lines] - newest_agreement, 0.0)
        multiplier_link = jnp.where(working_segment, multiplier_link + expected_condition - onward_refreshed, 0.0)
        feasibility_gap_total = jnp.sum(jnp.where(working_segment, (merged_pieces[:condition_lines] - newest_agreement) ** 2 + (expected_condition - onward_refreshed) ** 2, 0.0))
        dual_sum = RHO * RHO * jnp.sum(change_z * change_z)
        consensus = newest_agreement
        ahead_z = onward_refreshed
    state_traj = jnp.roll(merged_pieces[:condition_lines], offset, 1)
    input_traj = jnp.roll(merged_pieces[condition_lines:], offset, 1)
    consensus_out = jnp.roll(consensus, offset, 1)
    residual_norms = jnp.stack([jnp.sqrt(feasibility_gap_total), jnp.sqrt(dual_sum)]).astype(jnp.float32)
    return (state_traj, input_traj, consensus_out, residual_norms)
```

```python
import functools

import jax
import jax.numpy as jnp
from jax import lax
from jax.experimental import pallas as pl
from jax.experimental.pallas import tpu as pltpu
from jax.sharding import PartitionSpec as P

ITERS = 4
RHO = 1.0
LANES = 128
CHUNK = 512
ROWS = 64
NT = (((1,), (1,)), ((), ()))


def dot(a, b):
    return jnp.dot(a, b, preferred_element_type=jnp.float32)


def partner(me, k, n, sign):
    if n & (n - 1):
        return lax.rem(me + sign * k + n, n)
    other = me
    for bit in range(n.bit_length()):
        if (k >> bit) & 1:
            other = other + (1 - 2 * ((me // (1 << bit)) % 2)) * (1 << bit)
    return other


def kernel(
    n, width,
    a_hbm, b_hbm, k_hbm, cs_hbm, ci_hbm, start_ref, period_ref,
    x_out, u_out, z_out, norm_out,
    ab, gt, kkt, cs, ci, recv_s, recv_i, cpad, hsend, recv_h, hcol,
    negc, rhs, w, wb, pred, y, v, z, g, xo, uo, zo, part, recv_p,
    load_sem, own_sem, send_sem, recv_sem, out_sem,
):
    me = lax.axis_index("section")
    nx = a_hbm.shape[0]
    nu = b_hbm.shape[1]
    rs, ri = cs.shape[0], ci.shape[0]
    ext = width + LANES
    start = start_ref[0]
    period = period_ref[0]

    def cols(i):
        return pl.ds(pl.multiple_of(i * width, LANES), width)

    loads = [
        pltpu.make_async_copy(cs_hbm, cs, load_sem.at[0]),
        pltpu.make_async_copy(ci_hbm, ci, load_sem.at[1]),
        pltpu.make_async_copy(cs_hbm.at[:, cols(me)], recv_s.at[me], load_sem.at[2]),
        pltpu.make_async_copy(ci_hbm.at[:, cols(me)], recv_i.at[me], load_sem.at[3]),
        pltpu.make_async_copy(a_hbm, ab.at[:, pl.ds(0, nx)], load_sem.at[4]),
        pltpu.make_async_copy(b_hbm, ab.at[:, pl.ds(nx, nu)], load_sem.at[5]),
        pltpu.make_async_copy(k_hbm, kkt, load_sem.at[6]),
    ]
    for c in loads:
        c.start()

    barrier = pltpu.get_barrier_semaphore()
    for k in range(1, n):
        pl.semaphore_signal(barrier, inc=1, device_id={"section": partner(me, k, n, 1)})
    pl.semaphore_wait(barrier, n - 1)

    loads[0].wait()
    loads[1].wait()

    def copies(kind, k, incoming=False):
        to = partner(me, k, n, 1)
        if kind == 0:
            src, dst = cs.at[:, cols(to)], recv_s
        elif kind == 1:
            src, dst = ci.at[:, cols(to)], recv_i
        elif kind == 2:
            src, dst = hsend.at[to], recv_h
        else:
            src, dst = part, recv_p
        slot = partner(me, k, n, -1) if incoming else me
        return pltpu.make_async_remote_copy(
            src_ref=src, dst_ref=dst.at[slot], send_sem=send_sem.at[kind, k],
            recv_sem=recv_sem.at[kind, slot], device_id={"section": to},
        )

    order = range(n - 1, 0, -1)
    for k in order:
        copies(0, k).start()
        copies(1, k).start()

    row = lax.broadcasted_iota(jnp.int32, (n * 8, 1), 0)
    block = row // 8 - start
    block = jnp.where(block < 0, block + n, block)
    item = row % 8
    end = jnp.minimum(period - block * width, width)
    ahead = block * width + end + item
    ahead = jnp.where(ahead >= period, ahead - period, ahead)
    behind = block * width + item - 8
    behind = jnp.where(behind < 0, behind + period, behind)
    place = jnp.where(item < ITERS, ahead, behind) + start * width
    place = jnp.where(place >= n * width, place - n * width, place)

    cpad[...] = jnp.zeros_like(cpad)

    def pick(j, total):
        at = pl.ds(pl.multiple_of(j * CHUNK, CHUNK), CHUNK)
        cpad[pl.ds(0, rs), :] = cs[:, at]
        cpad[pl.ds(rs, ri), :] = ci[:, at]
        column = lax.broadcasted_iota(jnp.int32, (n * 8, CHUNK), 1) + j * CHUNK
        onehot = jnp.where(column == place, 1.0, 0.0).astype(jnp.bfloat16)
        rest = cpad[...]
        for _ in range(3):
            piece = rest.astype(jnp.bfloat16)
            rest = rest - piece.astype(jnp.float32)
            total = total + lax.dot_general(onehot, piece, NT, preferred_element_type=jnp.float32)
        return total

    picked = lax.fori_loop(
        0, cs.shape[1] // CHUNK, pick, jnp.zeros((n * 8, LANES), jnp.float32)
    )
    hsend[...] = picked.reshape(n, 8, LANES)
    own_halo = pltpu.make_async_copy(hsend.at[me], recv_h.at[me], own_sem.at[0])
    own_halo.start()
    for k in order:
        copies(2, k).start()

    loads[4].wait()
    loads[5].wait()
    loads[6].wait()
    gt[...] = ab[...].T

    loads[2].wait()
    loads[3].wait()
    own_halo.wait()
    for kind in (0, 1, 2):
        for k in order:
            copies(kind, k, True).wait_recv()

    flipped = recv_h[...].reshape(n * 8, LANES).T
    for s in range(n):
        tile = s * 8 // LANES * LANES
        piece = flipped[:, tile:tile + LANES]
        if s * 8 - tile:
            piece = pltpu.roll(piece, LANES - (s * 8 - tile), 1)
        hcol[pl.ds(s * rs, rs), :] = piece[:rs]
        hcol[pl.ds(nx + s * ri, ri), :] = piece[rs:rs + ri]

    mine = me - start
    mine = jnp.where(mine < 0, mine + n, mine)
    finish = jnp.minimum(period - mine * width, width)
    lane = lax.broadcasted_iota(jnp.int32, (1, LANES), 1)

    for s in range(n):
        negc[pl.ds(s * rs, rs), pl.ds(0, width)] = -recv_s[s]
        negc[pl.ds(nx + s * ri, ri), pl.ds(0, width)] = -recv_i[s]
    for r in range(0, nx + nu, ROWS):
        at = pl.ds(r, ROWS)
        h = -hcol[at, :]
        back = pltpu.roll(h, LANES - 8, 1)
        fills = [jnp.broadcast_to(h[:, i:i + 1], (ROWS, LANES)) for i in range(ITERS)]
        for t in range(0, ext, LANES):
            if t < width:
                value = negc[at, pl.ds(t, LANES)]
            else:
                value = jnp.where(lane >= LANES - ITERS, back, 0.0)
            for i in range(ITERS):
                value = jnp.where(lane + t == finish + i, fills[i], value)
            negc[at, pl.ds(t, LANES)] = value
            rhs[at, pl.ds(t, LANES)] = value.astype(jnp.bfloat16)

    ids = mine * width + lax.broadcasted_iota(jnp.int32, (1, width), 1)
    active = ids < period
    primal = jnp.zeros((8, LANES), jnp.float32)
    dual = jnp.zeros((8, LANES), jnp.float32)

    def fold(value):
        total = jnp.zeros((8, LANES), jnp.float32)
        for a in range(0, value.shape[0], 8):
            for b in range(0, value.shape[1], LANES):
                total = total + value[a:a + 8, b:b + LANES]
        return total

    for it in range(ITERS):
        last = it == ITERS - 1
        if it > 0:
            w[...] = dot(gt[...], g[...])
            for r in range(0, nx + nu, ROWS):
                at = pl.ds(r, ROWS)
                if r < nx:
                    value = negc[at, :] + RHO * (z[at, :] - y[at, :]) + RHO * w[at, :]
                else:
                    value = negc[at, :] + RHO * w[at, :]
                rhs[at, :] = value.astype(jnp.bfloat16)
        w[...] = dot(kkt[...], rhs[...])
        for r in range(0, nx + nu, ROWS):
            at = pl.ds(r, ROWS)
            wb[at, :] = w[at, :].astype(jnp.bfloat16)
        pred[...] = dot(ab[...], wb[...])
        for r in range(0, nx, ROWS):
            at = pl.ds(r, ROWS)
            x = w[at, :]
            q = pred[at, :]
            own = x + y[at, :] if it else x
            link = q + v[at, :] if it else q
            znew = 0.5 * (own + pltpu.roll(link, 1, 1))
            znext = pltpu.roll(znew, ext - 1, 1)
            if not last:
                y[at, :] = own - znew
                vnew = link - znext
                v[at, :] = vnew
                g[at, :] = (znext - vnew).astype(jnp.bfloat16)
                z[at, :] = znew
            else:
                miss = (x - znew) ** 2 + (q - znext) ** 2
                primal = primal + fold(jnp.where(active, miss[:, :width], 0.0))
                change = znew - z[at, :] if it else znew
                dual = dual + fold(jnp.where(active, (change * change)[:, :width], 0.0))
                xo[at, :] = jnp.where(active, x[:, :width], 0.0)
                zo[at, :] = jnp.where(active, znew[:, :width], 0.0)
    part[pl.ds(0, 8), :] = primal
    part[pl.ds(8, 8), :] = RHO * RHO * dual
    recv_p[me] = part[...]
    for k in order:
        copies(3, k).start()
    for r in range(0, nu, ROWS):
        uo[pl.ds(r, ROWS), :] = jnp.where(active, w[pl.ds(nx + r, ROWS), pl.ds(0, width)], 0.0)
    outs = [
        pltpu.make_async_copy(xo, x_out, out_sem.at[0]),
        pltpu.make_async_copy(uo, u_out, out_sem.at[1]),
        pltpu.make_async_copy(zo, z_out, out_sem.at[2]),
    ]
    for c in outs:
        c.start()
    for k in order:
        copies(3, k, True).wait_recv()
    total = recv_p[0]
    for s in range(1, n):
        total = total + recv_p[s]
    top = jnp.sqrt(jnp.broadcast_to(jnp.sum(total[:8], keepdims=True), (8, LANES)))
    low = jnp.sqrt(jnp.broadcast_to(jnp.sum(total[8:], keepdims=True), (8, LANES)))
    norm_out[0] = jnp.max(top)
    norm_out[1] = jnp.max(low)
    for c in outs:
        c.wait()
    for kind in (0, 1, 2, 3):
        for k in order:
            copies(kind, k).wait_send()


def local(a, b, kkt, lin_state, lin_input, block_start, period):
    n = lax.axis_size("section")
    width = lin_state.shape[1] // n
    ext = width + LANES
    nx, nu = b.shape
    nw = nx + nu
    rs, ri = lin_state.shape[0], lin_input.shape[0]
    f32, bf16 = jnp.float32, jnp.bfloat16
    anyspec = pl.BlockSpec(memory_space=pl.ANY)
    smem = pl.BlockSpec(memory_space=pltpu.SMEM)
    vmem = pltpu.VMEM
    return pl.pallas_call(
        functools.partial(kernel, n, width),
        name="admm",
        out_shape=(
            jax.ShapeDtypeStruct((nx, width), f32),
            jax.ShapeDtypeStruct((nu, width), f32),
            jax.ShapeDtypeStruct((nx, width), f32),
            jax.ShapeDtypeStruct((2,), f32),
        ),
        in_specs=[anyspec] * 5 + [smem] * 2,
        out_specs=(anyspec, anyspec, anyspec, smem),
        scratch_shapes=[
            vmem((nx, nw), bf16), vmem((nw, nx), bf16), vmem((nw, nw), bf16),
            vmem(lin_state.shape, f32), vmem(lin_input.shape, f32),
            vmem((n, rs, width), f32), vmem((n, ri, width), f32),
            vmem((LANES, CHUNK), f32),
            vmem((n, 8, LANES), f32), vmem((n, 8, LANES), f32), vmem((nw, LANES), f32),
            vmem((nw, ext), f32), vmem((nw, ext), bf16), vmem((nw, ext), f32),
            vmem((nw, ext), bf16), vmem((nx, ext), f32),
            vmem((nx, ext), f32), vmem((nx, ext), f32), vmem((nx, ext), f32),
            vmem((nx, ext), bf16),
            vmem((nx, width), f32), vmem((nu, width), f32), vmem((nx, width), f32),
            vmem((16, LANES), f32), vmem((n, 16, LANES), f32),
            pltpu.SemaphoreType.DMA((7,)), pltpu.SemaphoreType.DMA((1,)),
            pltpu.SemaphoreType.DMA((4, n)), pltpu.SemaphoreType.DMA((4, n)),
            pltpu.SemaphoreType.DMA((3,)),
        ],
        compiler_params=pltpu.CompilerParams(
            collective_id=0, has_side_effects=True, vmem_limit_bytes=48 * 1024 * 1024
        ),
    )(a, b, kkt, lin_state, lin_input, block_start, period)


def solution(mesh):
    return jax.shard_map(
        local,
        mesh=mesh,
        in_specs=(
            P("plant", None),
            P("plant", None),
            P("plant", None),
            P(("plant", "section"), None),
            P(("plant", "section"), None),
            P("plant"),
            P("plant"),
        ),
        out_specs=(P("plant", "section"), P("plant", "section"), P("plant", "section"), P("plant")),
        check_vma=False,
    )
```

```python
import functools

import jax
import jax.numpy as jnp
from jax import lax
from jax.experimental import pallas as pl
from jax.experimental.pallas import tpu as pltpu
from jax.sharding import PartitionSpec as P

ITERS = 4
RHO = 1.0
LANES = 128
CHUNK = 512
ROWS = 64
PARTS = 2
NT = (((1,), (1,)), ((), ()))


def dot(a, b):
    return jnp.dot(a, b, preferred_element_type=jnp.float32)


def partner(me, k, n, sign):
    if n & (n - 1):
        return lax.rem(me + sign * k + n, n)
    other = me
    for bit in range(n.bit_length()):
        if (k >> bit) & 1:
            other = other + (1 - 2 * ((me // (1 << bit)) % 2)) * (1 << bit)
    return other


def kernel(
    n, width,
    a_hbm, b_hbm, k_hbm, cs_hbm, ci_hbm, start_ref, period_ref,
    x_out, u_out, z_out, norm_out,
    ab, gt, kkt, cs, ci, recv_s, recv_i, cpad, hsend, recv_h, hcol,
    negc, rhs, w, wb, pred, y, v, z, g, xo, uo, zo, part, recv_p,
    load_sem, own_sem, send_sem, recv_sem, out_sem,
):
    me = lax.axis_index("section")
    nx = a_hbm.shape[0]
    nu = b_hbm.shape[1]
    rs, ri = cs.shape[0], ci.shape[0]
    pw = width // PARTS
    ext = pw + LANES
    shift = LANES // PARTS
    start = start_ref[0]
    period = period_ref[0]

    def cols(i, h):
        return pl.ds(pl.multiple_of(i * width + h * pw, LANES), pw)

    loads = [
        pltpu.make_async_copy(cs_hbm, cs, load_sem.at[0]),
        pltpu.make_async_copy(ci_hbm, ci, load_sem.at[1]),
        pltpu.make_async_copy(a_hbm, ab.at[:, pl.ds(0, nx)], load_sem.at[2]),
        pltpu.make_async_copy(b_hbm, ab.at[:, pl.ds(nx, nu)], load_sem.at[3]),
        pltpu.make_async_copy(k_hbm, kkt, load_sem.at[4]),
    ]
    for h in range(PARTS):
        loads += [
            pltpu.make_async_copy(
                cs_hbm.at[:, cols(me, h)], recv_s.at[h, me], load_sem.at[5 + 2 * h]
            ),
            pltpu.make_async_copy(
                ci_hbm.at[:, cols(me, h)], recv_i.at[h, me], load_sem.at[6 + 2 * h]
            ),
        ]
    for c in loads:
        c.start()

    barrier = pltpu.get_barrier_semaphore()
    for k in range(1, n):
        pl.semaphore_signal(barrier, inc=1, device_id={"section": partner(me, k, n, 1)})
    pl.semaphore_wait(barrier, n - 1)

    loads[0].wait()
    loads[1].wait()

    def copies(kind, k, incoming=False):
        to = partner(me, k, n, 1)
        if kind == 0:
            src, dst = part, recv_p
        elif kind == 1:
            src, dst = hsend.at[to], recv_h
        elif kind % 2 == 0:
            src, dst = cs.at[:, cols(to, kind // 2 - 1)], recv_s.at[kind // 2 - 1]
        else:
            src, dst = ci.at[:, cols(to, kind // 2 - 1)], recv_i.at[kind // 2 - 1]
        slot = partner(me, k, n, -1) if incoming else me
        return pltpu.make_async_remote_copy(
            src_ref=src, dst_ref=dst.at[slot], send_sem=send_sem.at[kind, k],
            recv_sem=recv_sem.at[kind, slot], device_id={"section": to},
        )

    order = list(range(1, n // 2)) + list(range(n - 1, n // 2 - 1, -1))
    for k in order:
        copies(2, k).start()
        copies(3, k).start()

    row = lax.broadcasted_iota(jnp.int32, (n * PARTS * 8, 1), 0)
    block = row // (PARTS * 8) - start
    block = jnp.where(block < 0, block + n, block)
    base = block * width + (row // 8) % PARTS * pw
    item = row % 8
    end = jnp.minimum(period - base, pw)
    ahead = base + end + item
    ahead = jnp.where(ahead >= period, ahead - period, ahead)
    behind = base + item - 8
    behind = jnp.where(behind < 0, behind + period, behind)
    place = jnp.where(item < ITERS, ahead, behind) + start * width
    place = jnp.where(place >= n * width, place - n * width, place)

    cpad[...] = jnp.zeros_like(cpad)

    def pick(j, total):
        at = pl.ds(pl.multiple_of(j * CHUNK, CHUNK), CHUNK)
        cpad[pl.ds(0, rs), :] = cs[:, at]
        cpad[pl.ds(rs, ri), :] = ci[:, at]
        column = lax.broadcasted_iota(jnp.int32, (n * PARTS * 8, CHUNK), 1) + j * CHUNK
        onehot = jnp.where(column == place, 1.0, 0.0).astype(jnp.bfloat16)
        rest = cpad[...]
        for _ in range(3):
            piece = rest.astype(jnp.bfloat16)
            rest = rest - piece.astype(jnp.float32)
            total = total + lax.dot_general(onehot, piece, NT, preferred_element_type=jnp.float32)
        return total

    picked = lax.fori_loop(
        0, cs.shape[1] // CHUNK, pick, jnp.zeros((n * PARTS * 8, LANES), jnp.float32)
    )
    picked = picked.reshape(n, PARTS, 8, LANES)
    packed = picked[:, 0].reshape(n * 8, LANES)
    for h in range(1, PARTS):
        packed = packed + pltpu.roll(picked[:, h].reshape(n * 8, LANES), h * shift, 1)
    hsend[...] = packed.reshape(n, 8, LANES)
    own_halo = pltpu.make_async_copy(hsend.at[me], recv_h.at[me], own_sem.at[0])
    own_halo.start()
    for k in order:
        copies(1, k).start()
    for h in range(1, PARTS):
        for k in order:
            copies(2 + 2 * h, k).start()
            copies(3 + 2 * h, k).start()

    loads[2].wait()
    loads[3].wait()
    loads[4].wait()
    gt[...] = ab[...].T

    own_halo.wait()
    for k in order:
        copies(1, k, True).wait_recv()

    flipped = recv_h[...].reshape(n * 8, LANES).T
    for s in range(n):
        tile = s * 8 // LANES * LANES
        piece = flipped[:, tile:tile + LANES]
        if s * 8 - tile:
            piece = pltpu.roll(piece, LANES - (s * 8 - tile), 1)
        for h in range(PARTS):
            top = h * shift
            hcol[h, pl.ds(s * rs, rs), :] = piece[top:top + rs]
            hcol[h, pl.ds(nx + s * ri, ri), :] = piece[top + rs:top + rs + ri]

    mine = me - start
    mine = jnp.where(mine < 0, mine + n, mine)
    lane = lax.broadcasted_iota(jnp.int32, (1, LANES), 1)
    primal = jnp.zeros((8, LANES), jnp.float32)
    dual = jnp.zeros((8, LANES), jnp.float32)

    def fold(value):
        total = jnp.zeros((8, LANES), jnp.float32)
        for a in range(0, value.shape[0], 8):
            for b in range(0, value.shape[1], LANES):
                total = total + value[a:a + 8, b:b + LANES]
        return total

    for h in range(PARTS):
        base = mine * width + h * pw
        finish = jnp.minimum(period - base, pw)
        own_cols = pl.ds(h * pw, pw)
        loads[5 + 2 * h].wait()
        loads[6 + 2 * h].wait()
        for k in order:
            copies(2 + 2 * h, k, True).wait_recv()
            copies(3 + 2 * h, k, True).wait_recv()

        for s in range(n):
            negc[pl.ds(s * rs, rs), pl.ds(0, pw)] = -recv_s[h, s]
            negc[pl.ds(nx + s * ri, ri), pl.ds(0, pw)] = -recv_i[h, s]
        for r in range(0, nx + nu, ROWS):
            at = pl.ds(r, ROWS)
            halo = -hcol[h, at, :]
            back = pltpu.roll(halo, LANES - 8, 1)
            fills = [jnp.broadcast_to(halo[:, i:i + 1], (ROWS, LANES)) for i in range(ITERS)]
            for t in range(0, ext, LANES):
                if t < pw:
                    value = negc[at, pl.ds(t, LANES)]
                else:
                    value = jnp.where(lane >= LANES - ITERS, back, 0.0)
                for i in range(ITERS):
                    value = jnp.where(lane + t == finish + i, fills[i], value)
                negc[at, pl.ds(t, LANES)] = value
                rhs[at, pl.ds(t, LANES)] = value.astype(jnp.bfloat16)

        ids = base + lax.broadcasted_iota(jnp.int32, (1, pw), 1)
        active = ids < period
        for it in range(ITERS):
            last = it == ITERS - 1
            if it > 0:
                w[...] = dot(gt[...], g[...])
                for r in range(0, nx + nu, ROWS):
                    at = pl.ds(r, ROWS)
                    if r < nx:
                        value = negc[at, :] + RHO * (z[at, :] - y[at, :]) + RHO * w[at, :]
                    else:
                        value = negc[at, :] + RHO * w[at, :]
                    rhs[at, :] = value.astype(jnp.bfloat16)
            w[...] = dot(kkt[...], rhs[...])
            for r in range(0, nx + nu, ROWS):
                at = pl.ds(r, ROWS)
                wb[at, :] = w[at, :].astype(jnp.bfloat16)
            pred[...] = dot(ab[...], wb[...])
            for r in range(0, nx, ROWS):
                at = pl.ds(r, ROWS)
                x = w[at, :]
                q = pred[at, :]
                own = x + y[at, :] if it else x
                link = q + v[at, :] if it else q
                znew = 0.5 * (own + pltpu.roll(link, 1, 1))
                znext = pltpu.roll(znew, ext - 1, 1)
                if not last:
                    y[at, :] = own - znew
                    vnew = link - znext
                    v[at, :] = vnew
                    g[at, :] = (znext - vnew).astype(jnp.bfloat16)
                    z[at, :] = znew
                else:
                    miss = (x - znew) ** 2 + (q - znext) ** 2
                    primal = primal + fold(jnp.where(active, miss[:, :pw], 0.0))
                    change = znew - z[at, :] if it else znew
                    dual = dual + fold(jnp.where(active, (change * change)[:, :pw], 0.0))
                    xo[at, own_cols] = jnp.where(active, x[:, :pw], 0.0)
                    zo[at, own_cols] = jnp.where(active, znew[:, :pw], 0.0)
        for r in range(0, nu, ROWS):
            uo[pl.ds(r, ROWS), own_cols] = jnp.where(
                active, w[pl.ds(nx + r, ROWS), pl.ds(0, pw)], 0.0
            )
    part[pl.ds(0, 8), :] = primal
    part[pl.ds(8, 8), :] = RHO * RHO * dual
    recv_p[me] = part[...]
    for k in order:
        copies(0, k).start()
    outs = [
        pltpu.make_async_copy(xo, x_out, out_sem.at[0]),
        pltpu.make_async_copy(uo, u_out, out_sem.at[1]),
        pltpu.make_async_copy(zo, z_out, out_sem.at[2]),
    ]
    for c in outs:
        c.start()
    for k in order:
        copies(0, k, True).wait_recv()
    total = recv_p[0]
    for s in range(1, n):
        total = total + recv_p[s]
    top = jnp.sqrt(jnp.broadcast_to(jnp.sum(total[:8], keepdims=True), (8, LANES)))
    low = jnp.sqrt(jnp.broadcast_to(jnp.sum(total[8:], keepdims=True), (8, LANES)))
    norm_out[0] = jnp.max(top)
    norm_out[1] = jnp.max(low)
    for c in outs:
        c.wait()
    for kind in range(2 + 2 * PARTS):
        for k in order:
            copies(kind, k).wait_send()


def local(a, b, kkt, lin_state, lin_input, block_start, period):
    n = lax.axis_size("section")
    width = lin_state.shape[1] // n
    pw = width // PARTS
    ext = pw + LANES
    nx, nu = b.shape
    nw = nx + nu
    rs, ri = lin_state.shape[0], lin_input.shape[0]
    f32, bf16 = jnp.float32, jnp.bfloat16
    anyspec = pl.BlockSpec(memory_space=pl.ANY)
    smem = pl.BlockSpec(memory_space=pltpu.SMEM)
    vmem = pltpu.VMEM
    return pl.pallas_call(
        functools.partial(kernel, n, width),
        name="admm",
        out_shape=(
            jax.ShapeDtypeStruct((nx, width), f32),
            jax.ShapeDtypeStruct((nu, width), f32),
            jax.ShapeDtypeStruct((nx, width), f32),
            jax.ShapeDtypeStruct((2,), f32),
        ),
        in_specs=[anyspec] * 5 + [smem] * 2,
        out_specs=(anyspec, anyspec, anyspec, smem),
        scratch_shapes=[
            vmem((nx, nw), bf16), vmem((nw, nx), bf16), vmem((nw, nw), bf16),
            vmem(lin_state.shape, f32), vmem(lin_input.shape, f32),
            vmem((PARTS, n, rs, pw), f32), vmem((PARTS, n, ri, pw), f32),
            vmem((LANES, CHUNK), f32),
            vmem((n, 8, LANES), f32), vmem((n, 8, LANES), f32), vmem((PARTS, nw, LANES), f32),
            vmem((nw, ext), f32), vmem((nw, ext), bf16), vmem((nw, ext), f32),
            vmem((nw, ext), bf16), vmem((nx, ext), f32),
            vmem((nx, ext), f32), vmem((nx, ext), f32), vmem((nx, ext), f32),
            vmem((nx, ext), bf16),
            vmem((nx, width), f32), vmem((nu, width), f32), vmem((nx, width), f32),
            vmem((16, LANES), f32), vmem((n, 16, LANES), f32),
            pltpu.SemaphoreType.DMA((5 + 2 * PARTS,)), pltpu.SemaphoreType.DMA((1,)),
            pltpu.SemaphoreType.DMA((2 + 2 * PARTS, n)), pltpu.SemaphoreType.DMA((2 + 2 * PARTS, n)),
            pltpu.SemaphoreType.DMA((3,)),
        ],
        compiler_params=pltpu.CompilerParams(
            collective_id=0, has_side_effects=True, vmem_limit_bytes=62000000
        ),
    )(a, b, kkt, lin_state, lin_input, block_start, period)


def solution(mesh):
    return jax.shard_map(
        local,
        mesh=mesh,
        in_specs=(
            P("plant", None),
            P("plant", None),
            P("plant", None),
            P(("plant", "section"), None),
            P(("plant", "section"), None),
            P("plant"),
            P("plant"),
        ),
        out_specs=(P("plant", "section"), P("plant", "section"), P("plant", "section"), P("plant")),
        check_vma=False,
    )
```
